256 devices in a mesh: ep: 16 (over y, x), tp: 16 (over z, core).
Axes of the slice: x: 4, y: 4, z: 8, core: 2. Of those that a mesh axis runs over, the one named last changes fastest.
Arguments:
- tokens: bfloat16 [1024, 7168], P('ep'), may hold values from -6 to 6
- gate_scores: float32 [1024, 8], P('ep'), may hold values from 0.1 to 1
- expert_ids: int32 [1024, 8], P('ep'), may hold values from 0 to 31, all different within a row; in each aligned block of 64 rows (0 to 63, 64 to 127, ...) at most 24 rows name the same one
- gate_weight: bfloat16 [32, 7168, 2048], P('ep', None, 'tp'), may hold values from -0.0625 to 0.0625
- up_weight: bfloat16 [32, 7168, 2048], P('ep', None, 'tp'), may hold values from -0.0625 to 0.0625
- down_weight: bfloat16 [32, 2048, 7168], P('ep', 'tp'), may hold values from -0.125 to 0.125
Outputs:
- mixed: bfloat16 [1024, 7168], P('ep', 'tp')
The draws below stay inside these ranges and needn't reach their ends.
Inputs may be any that keep to these rules, and one draw needn't show every extreme that they name: `expert_ids`: each row names 8 different experts. Among the tokens of one group, no expert is named by more than 24 tokens, and in every draw some expert is named by exactly 24 of them.
All inputs are finite; a program needn't handle non-finite values.
Results may differ from the reference program's by a relative error of at most 0.02.
Values may be sent and summed in bfloat16 or wider, within the bound.
A program may use at most 192 MiB of HBM per device.

```python
import math
import jax
import jax.numpy as jnp
import numpy as np
from jax import lax

D = 7168
FF = 2048
TOPK = 8
TOK_DEV = 64
EXPERTS = 32
CAP = 24
TOKENS = 1024
N_EP = 16
N_TP = 16


def block_levels(own_key, dims, pieces, smallest, top_value):
    gain = 1.0
    for dim, shards_of in pieces:
        draws = jax.random.uniform(jax.random.fold_in(jax.random.fold_in(own_key, 6), dim), (shards_of,), jnp.float32, smallest / len(pieces), top_value / len(pieces))
        gain = gain * jnp.repeat(jnp.exp(draws), dims[dim] // shards_of).reshape((-1,) + (1,) * (len(dims) - 1 - dim))
    return gain


def shared_out(own_key, own, number, rows, amount, top, reach, slope):
    order = jax.random.permutation(own_key, amount)
    crowded, usual = load_shares(amount, rows * top, reach, slope, True), load_shares(amount, rows * top, reach, slope, False)
    places = jnp.arange(amount)

    def named(sizes, turn):
        used = int((sizes > 0).sum())
        fixed = max(1, used // 4)
        shifted = fixed + (places - fixed + turn * (used - fixed)) % max(1, amount - fixed)
        return jnp.zeros((amount,), jnp.int32).at[order[jnp.where(places < fixed, places, shifted)]].set(jnp.asarray(sizes, jnp.int32))

    sizes = jnp.where(number % 4 == 0, named(crowded, number // 4), named(usual, number - number // 4 - 1))
    mixed = jax.random.permutation(jax.random.fold_in(own, 3), amount)
    source_of, receiver = mixed[0:amount // 2 * 2:2], mixed[1:amount // 2 * 2:2]
    slack = jnp.minimum(sizes[source_of] - 1, reach - sizes[receiver]) // 2
    slack = jnp.where((source_of == order[0]) | (receiver == order[0]) | (sizes[receiver] == 0), 0, jnp.maximum(slack, 0))
    shifted = jax.random.randint(jax.random.fold_in(own, 4), (amount // 2,), 0, 1 << 20) % (slack + 1)
    sizes = sizes.at[source_of].add(-shifted).at[receiver].add(shifted)
    labels = jnp.searchsorted(jnp.cumsum(sizes), jnp.arange(rows * top), side="right").astype(jnp.int32)
    table = labels.reshape(top, rows).T
    table = table[jax.random.permutation(jax.random.fold_in(own, 1), rows)]
    turn = jax.random.randint(jax.random.fold_in(own, 2), (rows, 1), 0, top)
    return jnp.take_along_axis(table, (jnp.arange(top)[None, :] + turn) % top, axis=1)


def load_shares(count, total, bound, slope, full):
    weights = [(1 << 20) // math.isqrt(grade ** slope) + 1 for grade in range(1, count + 1)]
    largest = bound if full else min(bound, max(-(-total // count), total * weights[0] // sum(weights)))
    least = 1 if total - largest >= count - 1 else 0
    counts, surplus = [largest] + [least] * (count - 1), total - largest - least * (count - 1)
    while surplus > 0:
        free = [i for i in range(1, count) if counts[i] < largest] or [i for i in range(1, count) if counts[i] < bound]
        mass, remaining = sum([weights[i] for i in free]), surplus
        for i in free:
            more = min(bound - counts[i], max(1, remaining * weights[i] // mass), surplus)
            counts[i] = counts[i] + more
            surplus = surplus - more
    return np.array(counts)


def scatter_about(rng, dims, scale, most, cuts=(), kind=jnp.bfloat16):
    drawn = jax.random.normal(rng, dims, jnp.float32) * scale
    if len(cuts) > 0:
        drawn = block_levels(rng, dims, cuts, -0.22, 0.18) * drawn
    return jnp.clip(drawn, min=-most, max=most).astype(kind)


def setup_inputs(seed: int = 0) -> dict:
    splits = jax.random.split(jax.random.key(seed), 7)
    tokens = scatter_about(splits[0], (TOKENS, D), 1.0, 6.0, ((0, 16),))
    gate_scores = jnp.clip(jnp.exp(math.log(1.0) - 2.3025851 * jax.random.uniform(splits[1], (TOKENS, TOPK), jnp.float32) ** block_levels(splits[1], (TOKENS, TOPK), ((0, 16),), -0.2, 0.2)), 0.1, 1.0)
    expert_ids_keys = jax.random.split(jax.random.fold_in(splits[2], 1), TOKENS // TOK_DEV)
    expert_ids_turns = jax.random.permutation(jax.random.fold_in(splits[2], 3), TOKENS // TOK_DEV)
    expert_ids = jax.vmap(lambda own, number: shared_out(jax.random.fold_in(splits[2], 2), own, number, TOK_DEV, EXPERTS, TOPK, CAP, 2))(expert_ids_keys, expert_ids_turns).reshape((TOKENS, TOPK))
    gate_weight = scatter_about(splits[3], (EXPERTS, D, FF), D ** -0.5, 0.0625, ((0, 16), (2, 16)))
    up_weight = scatter_about(splits[4], (EXPERTS, D, FF), D ** -0.5, 0.0625, ((0, 16), (2, 16)))
    down_weight = scatter_about(splits[5], (EXPERTS, FF, D), FF ** -0.5, 0.125, ((0, 16), (1, 16)))
    return dict(tokens=tokens, gate_scores=gate_scores, expert_ids=expert_ids, gate_weight=gate_weight, up_weight=up_weight, down_weight=down_weight)


def tables(ids_group):
    expert_range = jnp.arange(EXPERTS).astype(jnp.int32)
    picked = jnp.sum((ids_group[:, :, None] == expert_range[None, None, :]).astype(jnp.int32), axis=1)
    rank = jnp.cumsum(picked, axis=0) - picked
    slot = jnp.take_along_axis(rank, ids_group, axis=1)
    token_range = jnp.arange(TOK_DEV).astype(jnp.int32)
    slot_range = jnp.arange(CAP).astype(jnp.int32)
    hits = (rank.T[:, None, :] == slot_range[None, :, None]) & (picked.T[:, None, :] > 0)
    found = jnp.any(hits, axis=2)
    index = jnp.where(found, jnp.sum(hits.astype(jnp.int32) * token_range[None, None, :], axis=2), TOK_DEV)
    return slot, index.astype(jnp.int32)


def reference(tokens, gate_scores, expert_ids, gate_weight, up_weight, down_weight):
    ids_grouped = expert_ids.reshape(N_EP, TOK_DEV, TOPK)
    slot, index = jax.vmap(tables)(ids_grouped)
    padded = jnp.concatenate([tokens.reshape(N_EP, TOK_DEV, D), jnp.zeros((N_EP, 1, D), jnp.bfloat16)], axis=1)
    width_part = FF // N_TP

    def expert_out(expert):
        chosen = jax.vmap(lambda block, where: block[where])(padded, index[:, expert])
        chosen = chosen.reshape(N_EP * CAP, D)
        gate = jnp.dot(chosen, gate_weight[expert], preferred_element_type=jnp.float32)
        upper = jnp.dot(chosen, up_weight[expert], preferred_element_type=jnp.float32)
        hidden = (jax.nn.silu(gate) * upper).astype(jnp.bfloat16)
        hidden_parts = hidden.reshape(N_EP * CAP, N_TP, width_part).astype(jnp.float32)
        down_parts = down_weight[expert].reshape(N_TP, width_part, D).astype(jnp.float32)
        partial_value = jnp.einsum("rjf,jfd->jrd", hidden_parts, down_parts).astype(jnp.bfloat16)
        partial_value = lax.optimization_barrier(partial_value)
        summed = jnp.sum(partial_value.astype(jnp.float32), axis=0)
        return summed.astype(jnp.bfloat16).reshape(N_EP, CAP, D)

    outputs = lax.map(expert_out, jnp.arange(EXPERTS).astype(jnp.int32))
    groups = (jnp.arange(TOKENS).astype(jnp.int32) // TOK_DEV)[:, None] * jnp.ones((1, TOPK), jnp.int32)
    flat_slot = slot.reshape(TOKENS, TOPK)
    picked_rows = outputs[expert_ids, groups, flat_slot]
    weights = 2.5 * gate_scores / jnp.sum(gate_scores, axis=1, keepdims=True)
    mixed = jnp.einsum("tk,tkd->td", weights, picked_rows.astype(jnp.float32))
    return mixed.astype(jnp.bfloat16)
```

```python
import jax
import jax.numpy as jnp
from jax import lax
from jax.experimental import pallas as pl
from jax.experimental.pallas import tpu as pltpu
from jax.sharding import Mesh
from jax.sharding import PartitionSpec as P

F32, BF16 = jnp.float32, jnp.bfloat16
HALF = 3584
PART = 1280
ZOFF = 2 * PART
NA, NB = 384, 256
COPIES = 224


def kernel(
    tok, score, ids, gate_w, up_w, down_w, out,
    xa, xb, xc, wgu, wd, acc, wsend, wrecv, wcol, hid,
    ca, cb, cc, r1a, r2a, t1a, t2a, za, r1b, r2b, t1b, t2b, zb, q1, q2, q3, q4, xcr,
    send, recv, loc,
):
    y, x = lax.axis_index("y"), lax.axis_index("x")
    z, c = lax.axis_index("z"), lax.axis_index("c")
    g = y * 4 + x
    oc = 1 - c

    def m4(v, d):
        return lax.rem(v + (4 + d), 4)

    def m8(v, d):
        return lax.rem(v + (8 + d), 8)

    def dev(dy=0, dx=0, dz=0):
        return (m4(y, dy), m4(x, dx), m8(z, dz), c)

    sibling = (y, x, z, oc)
    started = []

    def put(src, dst, device):
        n = len(started)
        copy = pltpu.make_async_remote_copy(
            src_ref=src, dst_ref=dst, send_sem=send.at[n], recv_sem=recv.at[n],
            device_id=device, device_id_type=pl.DeviceIdType.MESH,
        )
        copy.start()
        started.append(copy)
        return copy

    def lanes(start, size):
        return pl.ds(pl.multiple_of(start, 128), size)

    plane = [(dy, dx) for dy in range(4) for dx in range(4) if dy or dx]

    own = [
        pltpu.make_async_copy(tok.at[:, lanes(c * HALF + ZOFF + z * 128, 128)], xc.at[c, z, g], loc.at[0]),
        pltpu.make_async_copy(tok.at[:, lanes(c * HALF, PART)], xa.at[c, y, x], loc.at[1]),
        pltpu.make_async_copy(tok.at[:, lanes(c * HALF + PART, PART)], xb.at[c, x, y], loc.at[2]),
    ]
    loads = []
    for e in range(2):
        loads.append(pltpu.make_async_copy(gate_w.at[e], wgu.at[:, pl.ds(e * 256, 128)], loc.at[3 + 3 * e]))
        loads.append(pltpu.make_async_copy(up_w.at[e], wgu.at[:, pl.ds(e * 256 + 128, 128)], loc.at[4 + 3 * e]))
        loads.append(pltpu.make_async_copy(down_w.at[e], wd.at[c, pl.ds(e * 128, 128)], loc.at[5 + 3 * e]))
    for copy in own:
        copy.start()

    barrier = pltpu.get_barrier_semaphore()
    for dy, dx in plane:
        pl.semaphore_signal(barrier, inc=1, device_id=dev(dy, dx), device_id_type=pl.DeviceIdType.MESH)
    for d in range(1, 8):
        pl.semaphore_signal(barrier, inc=1, device_id=dev(dz=d), device_id_type=pl.DeviceIdType.MESH)
    pl.semaphore_signal(barrier, inc=1, device_id=sibling, device_id_type=pl.DeviceIdType.MESH)
    for copy in own:
        copy.wait()
    for copy in loads:
        copy.start()
    pl.semaphore_wait(barrier, 23)

    routes = (
        (xa, y, x, lambda d: dev(dx=d), lambda d: dev(dy=d), 0, lambda k, j: k * 4 + j),
        (xb, x, y, lambda d: dev(dy=d), lambda d: dev(dx=d), PART, lambda k, j: j * 4 + k),
    )
    piece = {s: put(xc.at[c, z, g], xc.at[c, z, g], dev(*s)) for s in plane}
    first, half1, full2, half2 = {}, {}, {}, {}
    for p, (buf, k, i, m1, m2, off, rows) in enumerate(routes):
        for d in (1, -1):
            first[p, d] = put(buf.at[c, k, i], buf.at[c, k, i], m1(d))
    for p, (buf, k, i, m1, m2, off, rows) in enumerate(routes):
        for d in (1, -1):
            full2[p, 0, d] = put(buf.at[c, k, i], buf.at[c, k, i], m2(d))
    down_sib = [put(down_w.at[e], wd.at[c, pl.ds(e * 128, 128)], sibling) for e in range(2)]

    lane = lax.broadcasted_iota(jnp.int32, (64, 128), 1)
    expert = jnp.where((lane & 7) < 2, (lane >> 3) * 2 + (lane & 7), -1)
    s = score[...]
    norm = 2.5 * s / jnp.sum(s, axis=1, keepdims=True)
    dense = jnp.zeros((64, 128), F32)
    for t in range(8):
        dense += jnp.where(ids[:, t : t + 1] == expert, norm[:, t : t + 1], 0.0)
    wsend[...] = jnp.concatenate([dense, jnp.zeros((64, 128), F32)], axis=0).T.reshape(16, 8, 128)
    acc[...] = jnp.zeros_like(acc)
    wrecv[g] = wsend[g]
    wput = []
    for dy, dx in plane:
        to = m4(y, dy) * 4 + m4(x, dx)
        wput.append(put(wsend.at[to], wrecv.at[g], dev(dy, dx)))

    def mul(p, h, k):
        buf, off, rows = routes[p][0], routes[p][5], routes[p][6]
        start = pl.multiple_of(h * HALF + off, 128)
        r = jnp.dot(buf[h, k].reshape(256, PART), wgu[pl.ds(start, PART), :], preferred_element_type=F32)
        for j in range(4):
            acc[rows(k, j)] += r[j * 64 : (j + 1) * 64]

    def mulz(h, zz):
        start = pl.multiple_of(h * HALF + ZOFF + zz * 128, 128)

        @pl.loop(0, 4)
        def _(q):
            r = jnp.dot(xc[h, zz, pl.ds(q * 4, 4)].reshape(256, 128), wgu[pl.ds(start, 128), :], preferred_element_type=F32)
            acc[pl.ds(q * 4, 4)] += r.reshape(4, 64, 512)

    for s in plane:
        piece[s].wait_recv()
    zput = {(0, d): put(xc.at[c, z], xc.at[c, z], dev(dz=d)) for d in (1, -1)}
    zsib = [(put(xc.at[c, z], xc.at[c, z], sibling), z)]
    rsib = []

    for p, (buf, k, i, m1, m2, off, rows) in enumerate(routes):
        first[p, 1].wait_recv()
        b = m4(i, -1)
        half1[p, 1] = put(buf.at[c, k, b, pl.ds(0, 32)], buf.at[c, k, b, pl.ds(0, 32)], m1(1))
        first[p, -1].wait_recv()
        b = m4(i, 1)
        half1[p, -1] = put(buf.at[c, k, b, pl.ds(32, 32)], buf.at[c, k, b, pl.ds(32, 32)], m1(-1))
    for b in (-1, 1):
        for p, (buf, k, i, m1, m2, off, rows) in enumerate(routes):
            for d in (1, -1):
                full2[p, b, d] = put(buf.at[c, k, m4(i, b)], buf.at[c, k, m4(i, b)], m2(d))
    for copy in loads:
        copy.wait()
    mulz(c, z)
    for copy in wput:
        copy.wait_recv()
    wt = wrecv[...].reshape(128, 128).T
    wcol[...] = jnp.zeros_like(wcol)

    @pl.loop(0, 16)
    def _(q):
        for e in range(2):
            col = jnp.sum(jnp.where(lane == q * 8 + e, wt[:64], 0.0), axis=1, keepdims=True)
            wcol[q, :, e * 128 : (e + 1) * 128] = jnp.broadcast_to(col, (64, 128))

    def finish(p, k):
        buf = routes[p][0]
        rsib.append((put(buf.at[c, k], buf.at[c, k], sibling), p, k))
        mul(p, c, k)

    for p, (buf, k, i, m1, m2, off, rows) in enumerate(routes):
        half1[p, 1].wait_recv()
        half1[p, -1].wait_recv()
        for d in (1, -1):
            full2[p, 2, d] = put(buf.at[c, k, m4(i, 2)], buf.at[c, k, m4(i, 2)], m2(d))
    for p in range(2):
        finish(p, routes[p][1])

    def pass_on(b):
        for p, (buf, k, i, m1, m2, off, rows) in enumerate(routes):
            full2[p, b, 1].wait_recv()
            ref = buf.at[c, m4(k, -1), m4(i, b), pl.ds(0, 32)]
            half2[p, b, 1] = put(ref, ref, m2(1))
            full2[p, b, -1].wait_recv()
            ref = buf.at[c, m4(k, 1), m4(i, b), pl.ds(32, 32)]
            half2[p, b, -1] = put(ref, ref, m2(-1))

    def z_step(t):
        for d in (1, -1):
            zput[t - 1, d].wait_recv()
            zz = m8(z, -d * t)
            if t < 3:
                zput[t, d] = put(xc.at[c, zz], xc.at[c, zz], dev(dz=d))
            elif t == 3:
                part = pl.ds(0 if d == 1 else 8, 8)
                zput[t, d] = put(xc.at[c, zz, part], xc.at[c, zz, part], dev(dz=d))
            if t < 4:
                zsib.append((put(xc.at[c, zz], xc.at[c, zz], sibling), zz))
                mulz(c, zz)
        if t == 4:
            zz = m8(z, 4)
            zsib.append((put(xc.at[c, zz], xc.at[c, zz], sibling), zz))
            mulz(c, zz)

    def from_sib(n):
        copy, p, k = rsib[n]
        copy.wait_recv()
        mul(p, oc, k)

    def z_from_sib(n):
        copy, zz = zsib[n]
        copy.wait_recv()
        mulz(oc, zz)

    pass_on(0)
    z_step(1)
    z_from_sib(0)
    from_sib(0)
    from_sib(1)
    pass_on(-1)
    z_from_sib(1)
    z_from_sib(2)
    z_step(2)
    pass_on(1)
    z_from_sib(3)
    z_from_sib(4)
    pass_on(2)
    for p in range(2):
        finish(p, m4(routes[p][1], -1))
        finish(p, m4(routes[p][1], 1))
    z_step(3)
    for n in range(2, 6):
        from_sib(n)
    z_from_sib(5)
    z_from_sib(6)
    for p in range(2):
        for b in (0, -1, 1, 2):
            half2[p, b, 1].wait_recv()
            half2[p, b, -1].wait_recv()
        finish(p, m4(routes[p][1], 2))
    z_step(4)
    from_sib(6)
    from_sib(7)
    z_from_sib(7)

    @pl.loop(0, 16)
    def _(q):
        for e in range(2):
            gate = acc[q, :, e * 256 : e * 256 + 128]
            upper = acc[q, :, e * 256 + 128 : e * 256 + 256]
            value = gate / (1.0 + jnp.exp(-gate)) * upper * wcol[q, :, e * 128 : (e + 1) * 128]
            value = value.astype(BF16)
            hid[c, 0, q, :, e * 128 : (e + 1) * 128] = value[:32]
            hid[c, 1, q, :, e * 128 : (e + 1) * 128] = value[32:]

    hid_sib = put(hid.at[c], hid.at[c], sibling)
    for copy in down_sib:
        copy.wait_recv()
    hid_sib.wait_recv()

    ka, kb = y * oc + x * c, x * oc + y * c

    def along(first_axis, d):
        if first_axis:
            return (m4(y, 0) if d == 0 else lax.rem(y + 4 + d * c, 4), lax.rem(x + 4 + d * oc, 4), z, c)
        return (lax.rem(y + 4 + d * oc, 4), lax.rem(x + 4 + d * c, 4), z, c)

    def down(left, right, start, size):
        return jnp.dot(left, wd[0, :, lanes(start, size)], preferred_element_type=F32) + jnp.dot(
            right, wd[1, :, lanes(start, size)], preferred_element_type=F32
        )

    sums = (
        (ca, r1a, r2a, t1a, t2a, za, ka, kb, 0, NA, lambda d: along(False, d), lambda d: along(True, d),
         lambda k, j: (k * 4 + j) * oc + (j * 4 + k) * c),
        (cb, r1b, r2b, t1b, t2b, zb, kb, ka, 1, NB, lambda d: along(True, d), lambda d: along(False, d),
         lambda k, j: (j * 4 + k) * oc + (k * 4 + j) * c),
    )

    def row(p, k):
        buf, part, size, where = sums[p][0], sums[p][8], sums[p][9], sums[p][12]
        left = jnp.concatenate([hid[0, part, where(k, j)] for j in range(4)], axis=0)
        right = jnp.concatenate([hid[1, part, where(k, j)] for j in range(4)], axis=0)
        for zz in range(8):
            r = down(left, right, zz * 896 + c * 512, size)
            buf[k, :, :, zz * size : (zz + 1) * size] = r.reshape(4, 32, size).astype(BF16)

    side = (lax.broadcasted_iota(jnp.int32, (256, 128), 1) < 64) == (c == 0)

    def column(zz):
        @pl.loop(0, 2)
        def _(q):
            some = pl.ds(q * 8, 8)
            lo = [hid[n, 0, some].reshape(256, 256) for n in range(2)]
            hi = [hid[n, 1, some].reshape(256, 256) for n in range(2)]
            r = down(hi[0], hi[1], zz * 896 + c * 512 + 256, 128)
            cc[zz, some, :, 0:128] = r.reshape(8, 32, 128).astype(BF16)
            r_lo = down(lo[0], lo[1], zz * 896 + 384, 128)
            r_hi = down(hi[0], hi[1], zz * 896 + 384, 128)
            r = jnp.where(side, r_lo, pltpu.roll(r_hi, 64, 1))
            cc[zz, some, :, 128:256] = r.reshape(8, 32, 128).astype(BF16)

    def add(*refs):
        total = refs[0][...].astype(F32)
        for ref in refs[1:]:
            total += ref[...].astype(F32)
        refs[0][...] = total.astype(BF16)

    top, bottom = pl.ds(0, 16), pl.ds(16, 16)
    st1, ind, dep, st2, ind2, dep2 = {}, {}, {}, {}, {}, {}
    for p, (buf, r1, r2, t1, t2, zr, k, i, part, size, m2, m1, where) in enumerate(sums):
        row(p, m4(k, 2))
        st1[p, 1] = put(buf.at[m4(k, 2), :, top], r1.at[0], m2(1))
        st1[p, -1] = put(buf.at[m4(k, 2), :, bottom], r1.at[1], m2(-1))
    column(m8(z, 4))
    zq = {
        (1, 1): put(cc.at[m8(z, 4), pl.ds(0, 8)], q1.at[0], dev(dz=1)),
        (1, -1): put(cc.at[m8(z, 4), pl.ds(8, 8)], q1.at[1], dev(dz=-1)),
    }
    for p, (buf, r1, r2, t1, t2, zr, k, i, part, size, m2, m1, where) in enumerate(sums):
        row(p, m4(k, 1))
        ind[p, 1] = put(buf.at[m4(k, 1), :, bottom], r2.at[0, :, bottom], m2(1))
        row(p, m4(k, -1))
        ind[p, -1] = put(buf.at[m4(k, -1), :, top], r2.at[1, :, top], m2(-1))
    column(m8(z, 3))
    zi = {1: put(cc.at[m8(z, 3), pl.ds(8, 8)], q2.at[0, pl.ds(8, 8)], dev(dz=1))}
    column(m8(z, -3))
    zi[-1] = put(cc.at[m8(z, -3), pl.ds(0, 8)], q2.at[1, pl.ds(0, 8)], dev(dz=-1))

    zq[1, 1].wait_recv()
    add(cc.at[m8(z, 3), pl.ds(0, 8)], q1.at[0])
    zq[2, 1] = put(cc.at[m8(z, 3), pl.ds(0, 8)], q2.at[0, pl.ds(0, 8)], dev(dz=1))
    zq[1, -1].wait_recv()
    add(cc.at[m8(z, -3), pl.ds(8, 8)], q1.at[1])
    zq[2, -1] = put(cc.at[m8(z, -3), pl.ds(8, 8)], q2.at[1, pl.ds(8, 8)], dev(dz=-1))
    for t in (2, -2, 1, -1):
        column(m8(z, t))
    column(z)

    order = (2, 1, -1, 0)
    for p, (buf, r1, r2, t1, t2, zr, k, i, part, size, m2, m1, where) in enumerate(sums):
        st1[p, 1].wait_recv()
        st1[p, -1].wait_recv()
        for b in order:
            j = m4(i, b)
            add(buf.at[m4(k, 1), j, top], r1.at[0, j])
            dep[p, b, 1] = put(buf.at[m4(k, 1), j, top], r2.at[0, j, top], m2(1))
            add(buf.at[m4(k, -1), j, bottom], r1.at[1, j])
            dep[p, b, -1] = put(buf.at[m4(k, -1), j, bottom], r2.at[1, j, bottom], m2(-1))
    for p in range(2):
        row(p, sums[p][6])

    for n, d in enumerate((1, -1)):
        zi[d].wait_recv()
        zq[2, d].wait_recv()
        add(cc.at[m8(z, 2 * d)], q2.at[n])
        zq[3, d] = put(cc.at[m8(z, 2 * d)], q3.at[n], dev(dz=d))
    for n, d in enumerate((1, -1)):
        zq[3, d].wait_recv()
        add(cc.at[m8(z, d)], q3.at[n])
        zq[4, d] = put(cc.at[m8(z, d)], q4.at[n], dev(dz=d))

    for p in range(2):
        for d in (1, -1):
            ind[p, d].wait_recv()
    for b in order:
        for p, (buf, r1, r2, t1, t2, zr, k, i, part, size, m2, m1, where) in enumerate(sums):
            dep[p, b, 1].wait_recv()
            dep[p, b, -1].wait_recv()
            j = m4(i, b)
            add(buf.at[k, j], r2.at[0, j], r2.at[1, j])
            if b == 2:
                st2[p, 1] = put(buf.at[k, j, top], t1.at[0], m1(1))
                st2[p, -1] = put(buf.at[k, j, bottom], t1.at[1], m1(-1))
            elif b == 1:
                ind2[p, 1] = put(buf.at[k, j, bottom], t2.at[0, bottom], m1(1))
            elif b == -1:
                ind2[p, -1] = put(buf.at[k, j, top], t2.at[1, top], m1(-1))
    zq[4, 1].wait_recv()
    zq[4, -1].wait_recv()
    add(cc.at[z], q4.at[0], q4.at[1])
    last = []
    for n, (dy, dx) in enumerate(plane):
        to = m4(y, dy) * 4 + m4(x, dx)
        last.append(put(cc.at[z, to], xcr.at[n], dev(dy, dx)))
    for p, (buf, r1, r2, t1, t2, zr, k, i, part, size, m2, m1, where) in enumerate(sums):
        st2[p, 1].wait_recv()
        add(buf.at[k, m4(i, 1), top], t1.at[0])
        dep2[p, 1] = put(buf.at[k, m4(i, 1), top], t2.at[0, top], m1(1))
        st2[p, -1].wait_recv()
        add(buf.at[k, m4(i, -1), bottom], t1.at[1])
        dep2[p, -1] = put(buf.at[k, m4(i, -1), bottom], t2.at[1, bottom], m1(-1))
    for p, (buf, r1, r2, t1, t2, zr, k, i, part, size, m2, m1, where) in enumerate(sums):
        for d in (1, -1):
            ind2[p, d].wait_recv()
            dep2[p, d].wait_recv()
        add(buf.at[k, i], t2.at[0], t2.at[1])
        for d in range(1, 8):
            last.append(put(buf.at[k, i, :, lanes(m8(z, d) * size, size)], zr.at[d - 1], dev(dz=d)))
    for copy in last:
        copy.wait_recv()
    fa = ca[ka, kb, :, lanes(z * NA, NA)].astype(F32)
    fb = cb[kb, ka, :, lanes(z * NB, NB)].astype(F32)
    for d in range(7):
        fa += za[d].astype(F32)
        fb += zb[d].astype(F32)
    fc = cc[z, g].astype(F32)
    for n in range(15):
        fc += xcr[n].astype(F32)
    mixed = fc[:, 128:]
    turned = pltpu.roll(mixed, 64, 1)
    upper = jnp.concatenate([fb, fc[:, :128]], axis=1)

    @pl.when(c == 0)
    def _():
        out[0:32, :] = jnp.concatenate([fa, mixed], axis=1)[:, :448].astype(BF16)
        out[32:64, :] = jnp.concatenate([upper, turned], axis=1)[:, :448].astype(BF16)

    @pl.when(c == 1)
    def _():
        out[0:32, :] = pltpu.roll(jnp.concatenate([mixed, fa], axis=1), 448, 1)[:, :448].astype(BF16)
        out[32:64, :] = pltpu.roll(jnp.concatenate([turned, upper], axis=1), 448, 1)[:, :448].astype(BF16)

    for copy in started:
        copy.wait_send()


def local(tokens, gate_scores, expert_ids, gate_weight, up_weight, down_weight):
    vmem = pl.BlockSpec(memory_space=pltpu.VMEM)
    anywhere = pl.BlockSpec(memory_space=pl.ANY)

    def route(size):
        width = 8 * size
        return [
            pltpu.VMEM((2, 4, 16, width), BF16), pltpu.VMEM((2, 4, 32, width), BF16),
            pltpu.VMEM((2, 16, width), BF16), pltpu.VMEM((2, 32, width), BF16),
            pltpu.VMEM((7, 32, size), BF16),
        ]

    return pl.pallas_call(
        kernel,
        out_shape=jax.ShapeDtypeStruct((64, 448), BF16),
        in_specs=[anywhere, vmem, vmem, anywhere, anywhere, anywhere],
        out_specs=vmem,
        scratch_shapes=[
            pltpu.VMEM((2, 4, 4, 64, PART), BF16),
            pltpu.VMEM((2, 4, 4, 64, PART), BF16),
            pltpu.VMEM((2, 8, 16, 64, 128), BF16),
            pltpu.VMEM((7168, 512), BF16),
            pltpu.VMEM((2, 256, 7168), BF16),
            pltpu.VMEM((16, 64, 512), F32),
            pltpu.VMEM((16, 8, 128), F32),
            pltpu.VMEM((16, 8, 128), F32),
            pltpu.VMEM((16, 64, 256), F32),
            pltpu.VMEM((2, 2, 16, 32, 256), BF16),
            pltpu.VMEM((4, 4, 32, 8 * NA), BF16),
            pltpu.VMEM((4, 4, 32, 8 * NB), BF16),
            pltpu.VMEM((8, 16, 32, 256), BF16),
            *route(NA),
            *route(NB),
            pltpu.VMEM((2, 8, 32, 256), BF16),
            pltpu.VMEM((2, 16, 32, 256), BF16),
            pltpu.VMEM((2, 16, 32, 256), BF16),
            pltpu.VMEM((2, 16, 32, 256), BF16),
            pltpu.VMEM((15, 32, 256), BF16),
            pltpu.SemaphoreType.DMA((COPIES,)),
            pltpu.SemaphoreType.DMA((COPIES,)),
            pltpu.SemaphoreType.DMA((9,)),
        ],
        compiler_params=pltpu.CompilerParams(
            collective_id=0, has_side_effects=True, vmem_limit_bytes=66 * 1024 * 1024 - 2 * 1024 * 1024 - 65536
        ),
    )(tokens, gate_scores, expert_ids, gate_weight, up_weight, down_weight)


def solution(mesh):
    torus = Mesh(mesh.devices.reshape(4, 4, 8, 2), ("y", "x", "z", "c"))
    return jax.shard_map(
        local,
        mesh=torus,
        in_specs=(
            P(("y", "x"), None),
            P(("y", "x"), None),
            P(("y", "x"), None),
            P(("y", "x"), None, ("z", "c")),
            P(("y", "x"), None, ("z", "c")),
            P(("y", "x"), ("z", "c"), None),
        ),
        out_specs=P(("y", "x"), ("z", "c")),
        check_vma=False,
    )
```

```python
import jax
import jax.numpy as jnp
from jax import lax
from jax.experimental import pallas as pl
from jax.experimental.pallas import tpu as pltpu
from jax.sharding import Mesh
from jax.sharding import PartitionSpec as P

F32, BF16 = jnp.float32, jnp.bfloat16
HALF = 3584
PART = 1280
ZOFF = 2 * PART
WIDTHS = (384, 256)
CHUNKS = 2
TH = 64 // CHUNKS
RH = TH // 2
ROWS = ((0,), (-1, 1), (2,), (0, -1, 1), (0, -1, 1, 2))
PIECES = ((0, -1, 1, -2), (2, -3, 3, 4), (0, -1, 1, -2, 2, -3, 3, 4))
SENDS, RECVS = 25 * CHUNKS + 2, 59 * CHUNKS + 2


def kernel(
    tok, score, ids, gate_w, up_w, down_w, out,
    xa, xb, xc, wgu, wd, acc, wsend, wrecv, wcol, hid,
    ca, cb, cc, r1a, r2a, t1a, t2a, za, r1b, r2b, t1b, t2b, zb, q1, q2, q3, q4, xcr,
    send, recv, loc,
):
    y, x = lax.axis_index("y"), lax.axis_index("x")
    z, c = lax.axis_index("z"), lax.axis_index("c")
    g = y * 4 + x
    oc = 1 - c

    def m4(v, d):
        return lax.rem(v + (4 + d), 4)

    def m8(v, d):
        return lax.rem(v + (8 + d), 8)

    def dev(dy=0, dx=0, dz=0):
        return (m4(y, dy), m4(x, dx), m8(z, dz), c)

    sibling = (y, x, z, oc)
    counts = {"send": 0, "recv": 0}
    send_waits = []

    class Batch:
        def __init__(self, kind, ref):
            self.sem = (send if kind == "send" else recv).at[counts[kind]]
            self.ref = ref
            counts[kind] += 1
            assert counts[kind] <= (SENDS if kind == "send" else RECVS)
            if kind == "send":
                send_waits.append(self)

        def wait(self):
            pltpu.make_async_copy(self.ref, self.ref, self.sem).wait()

    def sends(ref):
        return Batch("send", ref)

    def recvs(ref):
        return Batch("recv", ref)

    def put(src, dst, device, out_batch, in_batch):
        pltpu.make_async_remote_copy(
            src_ref=src, dst_ref=dst, send_sem=out_batch.sem, recv_sem=in_batch.sem,
            device_id=device, device_id_type=pl.DeviceIdType.MESH,
        ).start()

    def lanes(start, size):
        return pl.ds(pl.multiple_of(start, 128), size)

    def mark(*_):
        pass

    plane = [(dy, dx) for dy in range(4) for dx in range(4) if dy or dx]
    everyone = range(CHUNKS)

    mark("a00_start")
    own = []
    for h in everyone:
        rows = pl.ds(h * TH, TH)
        own += [
            pltpu.make_async_copy(tok.at[rows, lanes(c * HALF + ZOFF + z * 128, 128)], xc.at[h, c, z, g], loc.at[3 * h]),
            pltpu.make_async_copy(tok.at[rows, lanes(c * HALF, PART)], xa.at[h, c, y * 4 + x], loc.at[3 * h + 1]),
            pltpu.make_async_copy(tok.at[rows, lanes(c * HALF + PART, PART)], xb.at[h, c, x * 4 + y], loc.at[3 * h + 2]),
        ]
    for copy in own:
        copy.start()
    barrier = pltpu.get_barrier_semaphore()
    for dy, dx in plane:
        pl.semaphore_signal(barrier, inc=1, device_id=dev(dy, dx), device_id_type=pl.DeviceIdType.MESH)
    for d in range(1, 8):
        pl.semaphore_signal(barrier, inc=1, device_id=dev(dz=d), device_id_type=pl.DeviceIdType.MESH)
    pl.semaphore_signal(barrier, inc=1, device_id=sibling, device_id_type=pl.DeviceIdType.MESH)
    for copy in own:
        copy.wait()
    loads = []
    wsem, dsem = loc.at[3 * CHUNKS], loc.at[3 * CHUNKS + 1]
    for e in range(2):
        pltpu.make_async_copy(gate_w.at[e], wgu.at[:, pl.ds(e * 256, 128)], wsem).start()
        pltpu.make_async_copy(up_w.at[e], wgu.at[:, pl.ds(e * 256 + 128, 128)], wsem).start()
    for e in range(2):
        pltpu.make_async_copy(down_w.at[e], wd.at[c, pl.ds(e * 128, 128)], dsem).start()
    mark("a01_barrier")
    pl.semaphore_wait(barrier, 23)

    w_out, w_in = sends(wsend.at[pl.ds(0, 15)]), recvs(wrecv.at[pl.ds(0, 15)])
    down_out, down_in = sends(wd.at[c]), recvs(wd.at[oc])

    def routing():
        line = lax.broadcasted_iota(jnp.int32, (128, 64), 0)
        expert = jnp.where((line & 7) < 2, (line >> 3) * 2 + (line & 7), -1)
        s = score[...]
        norm = 2.5 * s / jnp.sum(s, axis=0, keepdims=True)
        dense = jnp.zeros((128, 64), F32)
        for t in range(8):
            dense += jnp.where(ids[t : t + 1, :] == expert, norm[t : t + 1, :], 0.0)
        wsend[...] = jnp.zeros_like(wsend)
        wsend[:, :, 0:64] = dense.reshape(16, 8, 64)
        acc[...] = jnp.zeros_like(acc)
        wrecv[g] = wsend[g]
        for dy, dx in plane:
            put(wsend.at[m4(y, dy) * 4 + m4(x, dx)], wrecv.at[g], dev(dy, dx), w_out, w_in)
        for e in range(2):
            put(down_w.at[e], wd.at[c, pl.ds(e * 128, 128)], sibling, down_out, down_in)

    def routing_done():
        w_in.wait()
        wt = wrecv[...].reshape(128, 128).T
        lane = lax.broadcasted_iota(jnp.int32, (64, 128), 1)

        @pl.loop(0, 16)
        def _(q):
            for e in range(2):
                col = jnp.sum(jnp.where(lane == q * 8 + e, wt[:64], 0.0), axis=1, keepdims=True)
                wcol[q, :, e * 128 : (e + 1) * 128] = jnp.broadcast_to(col, (64, 128))

    class Gather:
        def __init__(self, h):
            self.h = h
            self.routes = (
                (xa.at[h], y, x, lambda d: dev(dx=d), lambda d: dev(dy=d), 0, lambda k, j: k * 4 + j),
                (xb.at[h], x, y, lambda d: dev(dy=d), lambda d: dev(dx=d), PART, lambda k, j: j * 4 + k),
            )
            self.xc = xc.at[h]
            two = [buf.at[c, pl.ds(0, 2)] for buf in (xa.at[h], xb.at[h])]
            self.block_out = [sends(buf.at[c, pl.ds(0, 15)]) for buf in (xa.at[h], xb.at[h])]
            self.row_out = [sends(buf.at[c]) for buf in (xa.at[h], xb.at[h])]
            self.piece_out = sends(xc.at[h, c, z, pl.ds(0, 15)])
            self.z_out = sends(xc.at[h, c, pl.ds(0, 7)])
            self.zsib_out = sends(xc.at[h, c])
            self.piece_in = recvs(xc.at[h, c, z, pl.ds(0, 15)])
            self.first_in = [recvs(ref) for ref in two]
            self.half1_in = [recvs(buf.at[c, 0]) for buf in (xa.at[h], xb.at[h])]
            self.full2_in = {(p, b): recvs(two[p]) for p in range(2) for b in (0, -1, 1, 2)}
            self.half2_in = [recvs(buf.at[c, pl.ds(0, 4)]) for buf in (xa.at[h], xb.at[h])]
            self.z_in = {(t, d): recvs(xc.at[h, c, 0] if t < 3 else xc.at[h, c, 0, pl.ds(0, 8)]) for t in range(4) for d in (1, -1)}
            self.row_in = {(p, n): recvs(buf.at[c, pl.ds(0, 8 if n == 1 else 4)]) for p, buf in enumerate((xa.at[h], xb.at[h])) for n in range(3)}
            self.zsib_in = [recvs(xc.at[h, c, pl.ds(0, n)]) for n in (4, 4)]

        def begin_pieces(self):
            for s in plane:
                ref = self.xc.at[c, z, g]
                put(ref, ref, dev(*s), self.piece_out, self.piece_in)

        def begin_first(self):
            for p, (buf, k, i, m1, m2, off, rows) in enumerate(self.routes):
                for d in (1, -1):
                    ref = buf.at[c, k * 4 + i]
                    put(ref, ref, m1(d), self.block_out[p], self.first_in[p])

        def begin_second(self):
            for p, (buf, k, i, m1, m2, off, rows) in enumerate(self.routes):
                for d in (1, -1):
                    ref = buf.at[c, k * 4 + i]
                    put(ref, ref, m2(d), self.block_out[p], self.full2_in[p, 0])

        def z_sib(self, zz, n):
            put(self.xc.at[c, zz], self.xc.at[c, zz], sibling, self.zsib_out, self.zsib_in[n])

        def pieces(self):
            self.piece_in.wait()
            ref = self.xc.at[c, z]
            for d in (1, -1):
                put(ref, ref, dev(dz=d), self.z_out, self.z_in[0, d])
            self.z_sib(z, 0)

        def firsts(self):
            for p, (buf, k, i, m1, m2, off, rows) in enumerate(self.routes):
                self.first_in[p].wait()
                ref = buf.at[c, k * 4 + m4(i, -1), pl.ds(0, RH)]
                put(ref, ref, m1(1), self.block_out[p], self.half1_in[p])
                ref = buf.at[c, k * 4 + m4(i, 1), pl.ds(RH, RH)]
                put(ref, ref, m1(-1), self.block_out[p], self.half1_in[p])
            for b in (-1, 1):
                for p in range(2):
                    self.forward(p, b)

        def forward(self, p, b):
            buf, k, i, m1, m2, off, rows = self.routes[p]
            ref = buf.at[c, k * 4 + m4(i, b)]
            for d in (1, -1):
                put(ref, ref, m2(d), self.block_out[p], self.full2_in[p, b])

        def row_sib(self, p, b, batch):
            buf, k = self.routes[p][:2]
            ref = buf.at[c, pl.ds(m4(k, b) * 4, 4)]
            put(ref, ref, sibling, self.row_out[p], batch)

        def halves(self):
            for p in range(2):
                self.half1_in[p].wait()
                self.forward(p, 2)
            for p in range(2):
                self.row_sib(p, 0, self.row_in[p, 0])

        def pass_on(self, b):
            for p, (buf, k, i, m1, m2, off, rows) in enumerate(self.routes):
                self.full2_in[p, b].wait()
                ref = buf.at[c, m4(k, -1) * 4 + m4(i, b), pl.ds(0, RH)]
                put(ref, ref, m2(1), self.block_out[p], self.half2_in[p])
                ref = buf.at[c, m4(k, 1) * 4 + m4(i, b), pl.ds(RH, RH)]
                put(ref, ref, m2(-1), self.block_out[p], self.half2_in[p])
                if b == 2:
                    self.row_sib(p, -1, self.row_in[p, 1])
                    self.row_sib(p, 1, self.row_in[p, 1])

        def z_step(self, t):
            for d in (1, -1):
                self.z_in[t - 1, d].wait()
                zz = m8(z, -d * t)
                if t < 3:
                    put(self.xc.at[c, zz], self.xc.at[c, zz], dev(dz=d), self.z_out, self.z_in[t, d])
                elif t == 3:
                    part = pl.ds(0 if d == 1 else 8, 8)
                    put(self.xc.at[c, zz, part], self.xc.at[c, zz, part], dev(dz=d), self.z_out, self.z_in[t, d])
                if t < 4:
                    self.z_sib(zz, {(1, 1): 0, (1, -1): 0, (2, 1): 0, (2, -1): 1, (3, 1): 1, (3, -1): 1}[t, d])
            if t == 4:
                self.z_sib(m8(z, 4), 1)

        def mul(self, p, src, part):
            buf, k, i, m1, m2, off, rows = self.routes[p]
            start = pl.multiple_of(src * HALF + off, 128)
            ks = [m4(k, b) for b in ROWS[part]]
            m = 4 * TH
            left = jnp.concatenate([buf[src, pl.ds(kk * 4, 4)].reshape(m, PART) for kk in ks], axis=0)

            @pl.loop(0, 2)
            def _(n):
                cols = lanes(n * 256, 256)
                r = jnp.dot(left, wgu[pl.ds(start, PART), cols], preferred_element_type=F32)
                for a, kk in enumerate(ks):
                    for j in range(4):
                        low = a * m + j * TH
                        acc[rows(kk, j), pl.ds(self.h * TH, TH), cols] += r[low : low + TH]

        def mulz(self, src, n):
            zs = [m8(z, b) for b in PIECES[n]]
            starts = [pl.multiple_of(src * HALF + ZOFF + zz * 128, 128) for zz in zs]
            per = 256 // TH

            @pl.loop(0, 16 // per)
            def _(q):
                some = pl.ds(q * per, per)
                left = jnp.concatenate([self.xc[src, zz, some].reshape(256, 128) for zz in zs], axis=1)
                right = jnp.concatenate([wgu[pl.ds(s, 128), :] for s in starts], axis=0)
                r = jnp.dot(left, right, preferred_element_type=F32)
                acc[some, pl.ds(self.h * TH, TH), :] += r.reshape(per, TH, 512)

        def late(self):
            for p in range(2):
                self.half2_in[p].wait()
                self.row_sib(p, 2, self.row_in[p, 2])

        def own_rows(self, n):
            for p in range(2):
                self.mul(p, c, n)

        def sib_rows(self, n):
            for p in range(2):
                for batch in ((0,), (1,), (2,), (0, 1), (0, 1, 2))[n]:
                    self.row_in[p, batch].wait()
                self.mul(p, oc, n)

        def sib_z(self, n):
            for batch in ((0,), (1,), (0, 1))[n]:
                self.zsib_in[batch].wait()
            self.mulz(oc, n)

        def hidden(self):
            h = self.h
            rows = pl.ds(h * TH, TH)

            @pl.loop(0, 16)
            def _(q):
                for e in range(2):
                    gate = acc[q, rows, e * 256 : e * 256 + 128]
                    upper = acc[q, rows, e * 256 + 128 : e * 256 + 256]
                    value = gate / (1.0 + jnp.exp(-gate)) * upper * wcol[q, rows, e * 128 : (e + 1) * 128]
                    value = value.astype(BF16)
                    hid[h, c, 0, q, :, e * 128 : (e + 1) * 128] = value[:RH]
                    hid[h, c, 1, q, :, e * 128 : (e + 1) * 128] = value[RH:]

            self.hid_in = recvs(hid.at[h, c])
            put(hid.at[h, c], hid.at[h, c], sibling, sends(hid.at[h, c]), self.hid_in)

    ka, kb = y * oc + x * c, x * oc + y * c

    def along(other, d):
        u, v = d * c, d * oc
        if other:
            return (lax.rem(y + 4 + u, 4), lax.rem(x + 4 + v, 4), z, c)
        return (lax.rem(y + 4 + v, 4), lax.rem(x + 4 + u, 4), z, c)

    def down(left, right, start, size):
        return jnp.dot(left, wd[0, :, lanes(start, size)], preferred_element_type=F32) + jnp.dot(
            right, wd[1, :, lanes(start, size)], preferred_element_type=F32
        )

    def add(*refs):
        total = refs[0][...].astype(F32)
        for ref in refs[1:]:
            total += ref[...].astype(F32)
        refs[0][...] = total.astype(BF16)

    order = (2, 1, -1, 0)
    side = (lax.broadcasted_iota(jnp.int32, (16 * RH, 128), 1) < 64) == (c == 0)

    class Sum:
        def __init__(self, h):
            self.h = h
            self.routes = (
                (ca.at[h], r1a.at[h], r2a.at[h], t1a.at[h], t2a.at[h], za.at[h], ka, kb, WIDTHS[0],
                 lambda d: along(False, d), lambda d: along(True, d)),
                (cb.at[h], r1b.at[h], r2b.at[h], t1b.at[h], t2b.at[h], zb.at[h], kb, ka, WIDTHS[1],
                 lambda d: along(True, d), lambda d: along(False, d)),
            )
            self.hid = hid.at[h]
            self.cc, self.q = cc.at[h], [None, q1.at[h], q2.at[h], q3.at[h], q4.at[h]]
            self.st1 = [(sends(r[1]), recvs(r[1])) for r in self.routes]
            self.ind = [(sends(r[2].at[0]), recvs(r[2].at[0])) for r in self.routes]
            self.dep_out = [sends(r[2].at[0]) for r in self.routes]
            self.dep_in = {(p, b): recvs(self.routes[p][2].at[0, 0]) for p in range(2) for b in order}
            self.st2 = [(sends(r[3]), recvs(r[3])) for r in self.routes]
            self.t2 = [(sends(r[4]), recvs(r[4])) for r in self.routes]
            self.zr = [(sends(r[5]), recvs(r[5])) for r in self.routes]
            self.q_out = [None] + [sends(q) for q in self.q[1:]]
            self.q_in = [None] + [(recvs(q.at[0]), recvs(q.at[1])) for q in self.q[1:]]
            self.xy = (sends(xcr.at[h]), recvs(xcr.at[h]))

        def cut(self, p):
            half = self.routes[p][8] * 4
            return pl.ds(0, half), pl.ds(half, half)

        def product(self, p):
            buf, size = self.routes[p][0], self.routes[p][8]
            left = self.hid[0, p].reshape(16 * RH, 256)
            right = self.hid[1, p].reshape(16 * RH, 256)
            for zz in range(8):
                r = down(left, right, zz * 896 + c * 512, size).astype(BF16)
                for q in range(16):
                    a, b = q // 4, q % 4
                    k, i = (a * oc + b * c, b * oc + a * c) if p == 0 else (b * oc + a * c, a * oc + b * c)
                    buf[k, i, :, zz * size : (zz + 1) * size] = r[q * RH : (q + 1) * RH]

        def begin(self, p):
            buf, r1, r2, t1, t2, zr, k, i, size, m2, m1 = self.routes[p]
            left, right = self.cut(p)
            self.product(p)
            put(buf.at[m4(k, 2), :, :, left], r1.at[0], m2(1), *self.st1[p])
            put(buf.at[m4(k, 2), :, :, right], r1.at[1], m2(-1), *self.st1[p])

        def independent(self, p):
            buf, r1, r2, t1, t2, zr, k, i, size, m2, m1 = self.routes[p]
            left, right = self.cut(p)
            put(buf.at[m4(k, 1), :, :, right], r2.at[0, :, :, right], m2(1), *self.ind[p])
            put(buf.at[m4(k, -1), :, :, left], r2.at[1, :, :, left], m2(-1), *self.ind[p])

        def columns(self, zs):
            lo = [self.hid[n, 0].reshape(16 * RH, 256) for n in range(2)]
            hi = [self.hid[n, 1].reshape(16 * RH, 256) for n in range(2)]

            def weights(*starts):
                return [jnp.concatenate([wd[n, :, lanes(s, 128)] for s in starts], axis=1) for n in range(2)]

            def dot(left, right):
                return jnp.dot(left[0], right[0], preferred_element_type=F32) + jnp.dot(left[1], right[1], preferred_element_type=F32)

            r_lo = dot(lo, weights(*(zz * 896 + 384 for zz in zs)))
            for n, zz in enumerate(zs):
                r = dot(hi, weights(zz * 896 + c * 512 + 256, zz * 896 + 384))
                self.cc[zz, :, :, 0:128] = r[:, :128].reshape(16, RH, 128).astype(BF16)
                r = jnp.where(side, r_lo[:, n * 128 : (n + 1) * 128], pltpu.roll(r[:, 128:], 64, 1))
                self.cc[zz, :, :, 128:256] = r.reshape(16, RH, 128).astype(BF16)

        def first_columns(self):
            first, second = pl.ds(0, 8), pl.ds(8, 8)
            cc_, q = self.cc, self.q
            self.columns((m8(z, 4), m8(z, 3)))
            put(cc_.at[m8(z, 4), first], q[1].at[0], dev(dz=1), self.q_out[1], self.q_in[1][0])
            put(cc_.at[m8(z, 4), second], q[1].at[1], dev(dz=-1), self.q_out[1], self.q_in[1][1])
            put(cc_.at[m8(z, 3), second], q[2].at[0, second], dev(dz=1), self.q_out[2], self.q_in[2][0])
            self.columns((m8(z, -3), m8(z, 2)))
            put(cc_.at[m8(z, -3), first], q[2].at[1, first], dev(dz=-1), self.q_out[2], self.q_in[2][1])

        def last_columns(self):
            self.columns((m8(z, -2), m8(z, 1)))
            self.columns((m8(z, -1), z))

        def z_second(self):
            first, second = pl.ds(0, 8), pl.ds(8, 8)
            cc_, q = self.cc, self.q
            self.q_in[1][0].wait()
            add(cc_.at[m8(z, 3), first], q[1].at[0])
            put(cc_.at[m8(z, 3), first], q[2].at[0, first], dev(dz=1), self.q_out[2], self.q_in[2][0])
            self.q_in[1][1].wait()
            add(cc_.at[m8(z, -3), second], q[1].at[1])
            put(cc_.at[m8(z, -3), second], q[2].at[1, second], dev(dz=-1), self.q_out[2], self.q_in[2][1])

        def z_next(self, t):
            for n, d in enumerate((1, -1)):
                self.q_in[t][n].wait()
                ref = self.cc.at[m8(z, d * (4 - t))]
                add(ref, self.q[t].at[n])
                put(ref, self.q[t + 1].at[n], dev(dz=d), self.q_out[t + 1], self.q_in[t + 1][n])

        def z_end(self):
            self.q_in[4][0].wait()
            self.q_in[4][1].wait()
            add(self.cc.at[z], self.q[4].at[0], self.q[4].at[1])
            for n, (dy, dx) in enumerate(plane):
                to = m4(y, dy) * 4 + m4(x, dx)
                put(self.cc.at[z, to], xcr.at[self.h, n], dev(dy, dx), *self.xy)

        def depend(self, p):
            buf, r1, r2, t1, t2, zr, k, i, size, m2, m1 = self.routes[p]
            left, right = self.cut(p)
            self.st1[p][1].wait()
            for b in order:
                j = m4(i, b)
                ref = buf.at[m4(k, 1), j, :, left]
                add(ref, r1.at[0, j])
                put(ref, r2.at[0, j, :, left], m2(1), self.dep_out[p], self.dep_in[p, b])
                ref = buf.at[m4(k, -1), j, :, right]
                add(ref, r1.at[1, j])
                put(ref, r2.at[1, j, :, right], m2(-1), self.dep_out[p], self.dep_in[p, b])

        def second(self, *blocks):
            for b in blocks:
                for p, (buf, r1, r2, t1, t2, zr, k, i, size, m2, m1) in enumerate(self.routes):
                    left, right = self.cut(p)
                    if b == 2:
                        self.ind[p][1].wait()
                    self.dep_in[p, b].wait()
                    j = m4(i, b)
                    add(buf.at[k, j], r2.at[0, j], r2.at[1, j])
                    if b == 2:
                        put(buf.at[k, j, :, left], t1.at[0], m1(1), *self.st2[p])
                        put(buf.at[k, j, :, right], t1.at[1], m1(-1), *self.st2[p])
                    elif b == 1:
                        put(buf.at[k, j, :, right], t2.at[0, :, right], m1(1), *self.t2[p])
                    elif b == -1:
                        put(buf.at[k, j, :, left], t2.at[1, :, left], m1(-1), *self.t2[p])

        def third(self):
            for p, (buf, r1, r2, t1, t2, zr, k, i, size, m2, m1) in enumerate(self.routes):
                left, right = self.cut(p)
                self.st2[p][1].wait()
                ref = buf.at[k, m4(i, 1), :, left]
                add(ref, t1.at[0])
                put(ref, t2.at[0, :, left], m1(1), *self.t2[p])
                ref = buf.at[k, m4(i, -1), :, right]
                add(ref, t1.at[1])
                put(ref, t2.at[1, :, right], m1(-1), *self.t2[p])

        def fourth(self):
            for p, (buf, r1, r2, t1, t2, zr, k, i, size, m2, m1) in enumerate(self.routes):
                self.t2[p][1].wait()
                add(buf.at[k, i], t2.at[0], t2.at[1])
                for d in (4, 3, -3, 2, -2, 1, -1):
                    n = d - 1 if d > 0 else d + 7
                    put(buf.at[k, i, :, lanes(m8(z, d) * size, size)], zr.at[n], dev(dz=d), *self.zr[p])

        def finish(self):
            h = self.h
            self.xy[1].wait()
            fc = self.cc[z, g].astype(F32)
            for n in range(15):
                fc += xcr[h, n].astype(F32)
            total = []
            for p, (buf, r1, r2, t1, t2, zr, k, i, size, m2, m1) in enumerate(self.routes):
                self.zr[p][1].wait()
                f = buf[k, i, :, lanes(z * size, size)].astype(F32)
                for d in range(7):
                    f += zr[d].astype(F32)
                total.append(f)
            fa, fb = total
            mixed = fc[:, 128:]
            turned = pltpu.roll(mixed, 64, 1)
            upper = jnp.concatenate([fb, fc[:, :128]], axis=1)
            one, two = slice(h * TH, h * TH + RH), slice(h * TH + RH, (h + 1) * TH)

            @pl.when(c == 0)
            def _():
                out[one, :] = jnp.concatenate([fa, mixed], axis=1)[:, :448].astype(BF16)
                out[two, :] = jnp.concatenate([upper, turned], axis=1)[:, :448].astype(BF16)

            @pl.when(c == 1)
            def _():
                out[one, :] = pltpu.roll(jnp.concatenate([mixed, fa], axis=1), 448, 1)[:, :448].astype(BF16)
                out[two, :] = pltpu.roll(jnp.concatenate([turned, upper], axis=1), 448, 1)[:, :448].astype(BF16)

    G = [Gather(h) for h in everyone]
    S = [Sum(h) for h in everyone]
    loads_in = [pltpu.make_async_copy(wgu, wgu, wsem), pltpu.make_async_copy(wd.at[c], wd.at[c], dsem)]

    def run(*steps):
        for n, step in enumerate(steps):
            call, rest = (step[0], step[1:]) if isinstance(step, tuple) else (step, ())
            mark(n, call, rest)
            call(*rest)

    def exchanged(h):
        G[h].hid_in.wait()

    a, b = G
    s, t = S
    run(
        a.begin_pieces, a.begin_first, a.begin_second, routing,
        a.pieces, a.firsts, b.begin_pieces, loads_in[0].wait, loads_in[1].wait,
        a.halves, (a.pass_on, 0), b.begin_first, (a.z_step, 1), (a.own_rows, 0),
        (a.pass_on, -1), routing_done, (a.pass_on, 1), b.begin_second, (a.sib_rows, 0), (a.z_step, 2), (a.pass_on, 2),
        b.pieces, (a.own_rows, 1), (a.mulz, c, 0), b.firsts, (a.sib_z, 0), (a.sib_rows, 1), (a.z_step, 3),
        a.late, (a.own_rows, 2), (b.z_step, 1), b.halves, (b.pass_on, 0), (a.z_step, 4), (a.mulz, c, 1),
        (b.pass_on, -1), (a.sib_rows, 2), (b.pass_on, 1), (a.sib_z, 1), a.hidden,
        (b.z_step, 2), (b.pass_on, 2), (b.own_rows, 3), down_in.wait, (exchanged, 0),
        s.first_columns, (s.begin, 0), (s.begin, 1), (s.independent, 0), (s.independent, 1), (b.z_step, 3), b.late,
        (b.mulz, c, 0), (b.sib_rows, 3), s.z_second, (b.own_rows, 2), s.last_columns, (b.z_step, 4),
        (b.mulz, c, 1), (b.sib_rows, 2), (s.depend, 0), (s.depend, 1), (s.z_next, 2), (b.sib_z, 2), b.hidden,
        (exchanged, 1), t.first_columns, (s.second, 2), (t.begin, 0), (s.second, 1, -1, 0), (t.begin, 1),
        (t.independent, 0), (t.independent, 1), t.last_columns, (s.z_next, 3), t.z_second, s.third, (t.depend, 0), (t.depend, 1),
        s.z_end, s.fourth, (t.z_next, 2), (t.second, 2), (t.second, 1), (t.z_next, 3), (t.second, -1, 0), t.third, t.z_end,
        t.fourth, s.finish, t.finish,
    )
    mark("b30_sends")
    for batch in send_waits:
        batch.wait()
    mark(None)


def local(tokens, gate_scores, expert_ids, gate_weight, up_weight, down_weight):
    vmem = pl.BlockSpec(memory_space=pltpu.VMEM)
    anywhere = pl.BlockSpec(memory_space=pl.ANY)

    def bf16(*shape):
        return pltpu.VMEM((CHUNKS, *shape), BF16)

    def route(size):
        w = 8 * size
        return [bf16(2, 4, RH, w // 2), bf16(2, 4, RH, w), bf16(2, RH, w // 2), bf16(2, RH, w), bf16(7, RH, size)]

    return pl.pallas_call(
        kernel,
        out_shape=jax.ShapeDtypeStruct((64, 448), BF16),
        in_specs=[anywhere, vmem, vmem, anywhere, anywhere, anywhere],
        out_specs=vmem,
        scratch_shapes=[
            bf16(2, 16, TH, PART),
            bf16(2, 16, TH, PART),
            bf16(2, 8, 16, TH, 128),
            pltpu.VMEM((7168, 512), BF16),
            pltpu.VMEM((2, 256, 7168), BF16),
            pltpu.VMEM((16, 64, 512), F32),
            pltpu.VMEM((16, 8, 128), F32),
            pltpu.VMEM((16, 8, 128), F32),
            pltpu.VMEM((16, 64, 256), F32),
            bf16(2, 2, 16, RH, 256),
            bf16(4, 4, RH, 8 * WIDTHS[0]),
            bf16(4, 4, RH, 8 * WIDTHS[1]),
            bf16(8, 16, RH, 256),
            *route(WIDTHS[0]),
            *route(WIDTHS[1]),
            bf16(2, 8, RH, 256),
            bf16(2, 16, RH, 256),
            bf16(2, 16, RH, 256),
            bf16(2, 16, RH, 256),
            bf16(15, RH, 256),
            pltpu.SemaphoreType.DMA((SENDS,)),
            pltpu.SemaphoreType.DMA((RECVS,)),
            pltpu.SemaphoreType.DMA((3 * CHUNKS + 2,)),
        ],
        compiler_params=pltpu.CompilerParams(
            collective_id=0, has_side_effects=True, vmem_limit_bytes=67043328
        ),
    )(tokens, gate_scores.T, expert_ids.T, gate_weight, up_weight, down_weight)


def solution(mesh):
    torus = Mesh(mesh.devices.reshape(4, 4, 8, 2), ("y", "x", "z", "c"))
    return jax.shard_map(
        local,
        mesh=torus,
        in_specs=(
            P(("y", "x"), None),
            P(("y", "x"), None),
            P(("y", "x"), None),
            P(("y", "x"), None, ("z", "c")),
            P(("y", "x"), None, ("z", "c")),
            P(("y", "x"), ("z", "c"), None),
        ),
        out_specs=P(("y", "x"), ("z", "c")),
        check_vma=False,
    )
```

```python
import jax
import jax.numpy as jnp
from jax import lax
from jax.experimental import pallas as pl
from jax.experimental.pallas import tpu as pltpu
from jax.sharding import Mesh
from jax.sharding import PartitionSpec as P

F32, BF16 = jnp.float32, jnp.bfloat16
HALF = 3584
PART = 1280
ZOFF = 2 * PART
WIDTHS = (384, 256)
CHUNKS = 2
TH = 64 // CHUNKS
RH = TH // 2
ROWS = ((0,), (-1, 1), (2,), (0, -1, 1), (0, -1, 1, 2))
PIECES = ((0, -1, 1, -2), (2, -3, 3, 4), (0, -1, 1, -2, 2, -3, 3, 4))
SENDS, RECVS = 25 * CHUNKS + 2, 59 * CHUNKS + 2


def kernel(
    tok, score, ids, gate_w, up_w, down_w, out,
    xa, xb, xc, wgu, wd, acc, wsend, wrecv, wcol, hid,
    ca, cb, cc, r1a, r2a, t1a, t2a, za, r1b, r2b, t1b, t2b, zb, q1, q2, q3, q4, xcr,
    send, recv, loc,
):
    y, x = lax.axis_index("y"), lax.axis_index("x")
    z, c = lax.axis_index("z"), lax.axis_index("c")
    g = y * 4 + x
    oc = 1 - c

    def m4(v, d):
        return lax.rem(v + (4 + d), 4)

    def m8(v, d):
        return lax.rem(v + (8 + d), 8)

    def dev(dy=0, dx=0, dz=0):
        return (m4(y, dy), m4(x, dx), m8(z, dz), c)

    sibling = (y, x, z, oc)
    counts = {"send": 0, "recv": 0}
    send_waits = []

    class Batch:
        def __init__(self, kind, ref):
            self.sem = (send if kind == "send" else recv).at[counts[kind]]
            self.ref = ref
            counts[kind] += 1
            assert counts[kind] <= (SENDS if kind == "send" else RECVS)
            if kind == "send":
                send_waits.append(self)

        def wait(self):
            pltpu.make_async_copy(self.ref, self.ref, self.sem).wait()

    def sends(ref):
        return Batch("send", ref)

    def recvs(ref):
        return Batch("recv", ref)

    def put(src, dst, device, out_batch, in_batch):
        pltpu.make_async_remote_copy(
            src_ref=src, dst_ref=dst, send_sem=out_batch.sem, recv_sem=in_batch.sem,
            device_id=device, device_id_type=pl.DeviceIdType.MESH,
        ).start()

    def lanes(start, size):
        return pl.ds(pl.multiple_of(start, 128), size)

    def mark(*_):
        pass

    plane = [(dy, dx) for dy in range(4) for dx in range(4) if dy or dx]
    everyone = range(CHUNKS)

    mark("a00_start")
    own = []
    for h in everyone:
        rows = pl.ds(h * TH, TH)
        own += [
            pltpu.make_async_copy(tok.at[rows, lanes(c * HALF + ZOFF + z * 128, 128)], xc.at[h, c, z, g], loc.at[3 * h]),
            pltpu.make_async_copy(tok.at[rows, lanes(c * HALF, PART)], xa.at[h, c, y * 4 + x], loc.at[3 * h + 1]),
            pltpu.make_async_copy(tok.at[rows, lanes(c * HALF + PART, PART)], xb.at[h, c, x * 4 + y], loc.at[3 * h + 2]),
        ]
    for copy in own:
        copy.start()
    barrier = pltpu.get_barrier_semaphore()
    for dy, dx in plane:
        pl.semaphore_signal(barrier, inc=1, device_id=dev(dy, dx), device_id_type=pl.DeviceIdType.MESH)
    for d in range(1, 8):
        pl.semaphore_signal(barrier, inc=1, device_id=dev(dz=d), device_id_type=pl.DeviceIdType.MESH)
    pl.semaphore_signal(barrier, inc=1, device_id=sibling, device_id_type=pl.DeviceIdType.MESH)
    for copy in own:
        copy.wait()
    loads = []
    wsem, dsem = loc.at[3 * CHUNKS], loc.at[3 * CHUNKS + 1]
    for e in range(2):
        pltpu.make_async_copy(gate_w.at[e], wgu.at[:, pl.ds(e * 256, 128)], wsem).start()
        pltpu.make_async_copy(up_w.at[e], wgu.at[:, pl.ds(e * 256 + 128, 128)], wsem).start()
    for e in range(2):
        pltpu.make_async_copy(down_w.at[e], wd.at[c, pl.ds(e * 128, 128)], dsem).start()
    mark("a01_barrier")
    pl.semaphore_wait(barrier, 23)

    w_out, w_in = sends(wsend.at[pl.ds(0, 15)]), recvs(wrecv.at[pl.ds(0, 15)])
    down_out, down_in = sends(wd.at[c]), recvs(wd.at[oc])

    def routing():
        line = lax.broadcasted_iota(jnp.int32, (128, 64), 0)
        expert = jnp.where((line & 7) < 2, (line >> 3) * 2 + (line & 7), -1)
        s = score[...]
        norm = 2.5 * s / jnp.sum(s, axis=0, keepdims=True)
        dense = jnp.zeros((128, 64), F32)
        for t in range(8):
            dense += jnp.where(ids[t : t + 1, :] == expert, norm[t : t + 1, :], 0.0)
        wsend[...] = jnp.zeros_like(wsend)
        wsend[:, :, 0:64] = dense.reshape(16, 8, 64)
        acc[...] = jnp.zeros_like(acc)
        wrecv[g] = wsend[g]
        for dy, dx in plane:
            put(wsend.at[m4(y, dy) * 4 + m4(x, dx)], wrecv.at[g], dev(dy, dx), w_out, w_in)
        for e in range(2):
            put(down_w.at[e], wd.at[c, pl.ds(e * 128, 128)], sibling, down_out, down_in)

    def routing_done():
        w_in.wait()
        wt = wrecv[...].reshape(128, 128).T
        lane = lax.broadcasted_iota(jnp.int32, (64, 128), 1)

        @pl.loop(0, 16)
        def _(q):
            for e in range(2):
                col = jnp.sum(jnp.where(lane == q * 8 + e, wt[:64], 0.0), axis=1, keepdims=True)
                wcol[q, :, e * 128 : (e + 1) * 128] = jnp.broadcast_to(col, (64, 128))

    class Gather:
        def __init__(self, h):
            self.h = h
            self.routes = (
                (xa.at[h], y, x, lambda d: dev(dx=d), lambda d: dev(dy=d), 0, lambda k, j: k * 4 + j),
                (xb.at[h], x, y, lambda d: dev(dy=d), lambda d: dev(dx=d), PART, lambda k, j: j * 4 + k),
            )
            self.xc = xc.at[h]
            two = [buf.at[c, pl.ds(0, 2)] for buf in (xa.at[h], xb.at[h])]
            self.block_out = [sends(buf.at[c, pl.ds(0, 15)]) for buf in (xa.at[h], xb.at[h])]
            self.row_out = [sends(buf.at[c]) for buf in (xa.at[h], xb.at[h])]
            self.piece_out = sends(xc.at[h, c, z, pl.ds(0, 15)])
            self.z_out = sends(xc.at[h, c, pl.ds(0, 7)])
            self.zsib_out = sends(xc.at[h, c])
            self.piece_in = recvs(xc.at[h, c, z, pl.ds(0, 15)])
            self.first_in = [recvs(ref) for ref in two]
            self.half1_in = [recvs(buf.at[c, 0]) for buf in (xa.at[h], xb.at[h])]
            self.full2_in = {(p, b): recvs(two[p]) for p in range(2) for b in (0, -1, 1, 2)}
            self.half2_in = [recvs(buf.at[c, pl.ds(0, 4)]) for buf in (xa.at[h], xb.at[h])]
            self.z_in = {(t, d): recvs(xc.at[h, c, 0] if t < 3 else xc.at[h, c, 0, pl.ds(0, 8)]) for t in range(4) for d in (1, -1)}
            self.row_in = {(p, n): recvs(buf.at[c, pl.ds(0, 8 if n == 1 else 4)]) for p, buf in enumerate((xa.at[h], xb.at[h])) for n in range(3)}
            self.zsib_in = [recvs(xc.at[h, c, pl.ds(0, n)]) for n in (4, 4)]

        def begin_pieces(self):
            for s in plane:
                ref = self.xc.at[c, z, g]
                put(ref, ref, dev(*s), self.piece_out, self.piece_in)

        def begin_first(self):
            for p, (buf, k, i, m1, m2, off, rows) in enumerate(self.routes):
                for d in (1, -1):
                    ref = buf.at[c, k * 4 + i]
                    put(ref, ref, m1(d), self.block_out[p], self.first_in[p])

        def begin_second(self):
            for p, (buf, k, i, m1, m2, off, rows) in enumerate(self.routes):
                for d in (1, -1):
                    ref = buf.at[c, k * 4 + i]
                    put(ref, ref, m2(d), self.block_out[p], self.full2_in[p, 0])

        def z_sib(self, zz, n):
            put(self.xc.at[c, zz], self.xc.at[c, zz], sibling, self.zsib_out, self.zsib_in[n])

        def pieces(self):
            self.piece_in.wait()
            ref = self.xc.at[c, z]
            for d in (1, -1):
                put(ref, ref, dev(dz=d), self.z_out, self.z_in[0, d])
            self.z_sib(z, 0)

        def firsts(self):
            for p, (buf, k, i, m1, m2, off, rows) in enumerate(self.routes):
                self.first_in[p].wait()
                ref = buf.at[c, k * 4 + m4(i, -1), pl.ds(0, RH)]
                put(ref, ref, m1(1), self.block_out[p], self.half1_in[p])
                ref = buf.at[c, k * 4 + m4(i, 1), pl.ds(RH, RH)]
                put(ref, ref, m1(-1), self.block_out[p], self.half1_in[p])
            for b in (-1, 1):
                for p in range(2):
                    self.forward(p, b)

        def forward(self, p, b):
            buf, k, i, m1, m2, off, rows = self.routes[p]
            ref = buf.at[c, k * 4 + m4(i, b)]
            for d in (1, -1):
                put(ref, ref, m2(d), self.block_out[p], self.full2_in[p, b])

        def row_sib(self, p, b, batch):
            buf, k = self.routes[p][:2]
            ref = buf.at[c, pl.ds(m4(k, b) * 4, 4)]
            put(ref, ref, sibling, self.row_out[p], batch)

        def halves(self):
            for p in range(2):
                self.half1_in[p].wait()
                self.forward(p, 2)
            for p in range(2):
                self.row_sib(p, 0, self.row_in[p, 0])

        def pass_on(self, b):
            for p, (buf, k, i, m1, m2, off, rows) in enumerate(self.routes):
                self.full2_in[p, b].wait()
                ref = buf.at[c, m4(k, -1) * 4 + m4(i, b), pl.ds(0, RH)]
                put(ref, ref, m2(1), self.block_out[p], self.half2_in[p])
                ref = buf.at[c, m4(k, 1) * 4 + m4(i, b), pl.ds(RH, RH)]
                put(ref, ref, m2(-1), self.block_out[p], self.half2_in[p])
                if b == 2:
                    self.row_sib(p, -1, self.row_in[p, 1])
                    self.row_sib(p, 1, self.row_in[p, 1])

        def z_step(self, t):
            for d in (1, -1):
                self.z_in[t - 1, d].wait()
                zz = m8(z, -d * t)
                if t < 3:
                    put(self.xc.at[c, zz], self.xc.at[c, zz], dev(dz=d), self.z_out, self.z_in[t, d])
                elif t == 3:
                    part = pl.ds(0 if d == 1 else 8, 8)
                    put(self.xc.at[c, zz, part], self.xc.at[c, zz, part], dev(dz=d), self.z_out, self.z_in[t, d])
                if t < 4:
                    self.z_sib(zz, {(1, 1): 0, (1, -1): 0, (2, 1): 0, (2, -1): 1, (3, 1): 1, (3, -1): 1}[t, d])
            if t == 4:
                self.z_sib(m8(z, 4), 1)

        def mul(self, p, src, part):
            buf, k, i, m1, m2, off, rows = self.routes[p]
            start = pl.multiple_of(src * HALF + off, 128)
            ks = [m4(k, b) for b in ROWS[part]]
            m = 4 * TH
            left = jnp.concatenate([buf[src, pl.ds(kk * 4, 4)].reshape(m, PART) for kk in ks], axis=0)

            @pl.loop(0, 2)
            def _(n):
                cols = lanes(n * 256, 256)
                r = jnp.dot(left, wgu[pl.ds(start, PART), cols], preferred_element_type=F32)
                for a, kk in enumerate(ks):
                    for j in range(4):
                        low = a * m + j * TH
                        acc[rows(kk, j), pl.ds(self.h * TH, TH), cols] += r[low : low + TH]

        def mulz(self, src, n):
            zs = [m8(z, b) for b in PIECES[n]]
            starts = [pl.multiple_of(src * HALF + ZOFF + zz * 128, 128) for zz in zs]
            per = 256 // TH

            @pl.loop(0, 16 // per)
            def _(q):
                some = pl.ds(q * per, per)
                left = jnp.concatenate([self.xc[src, zz, some].reshape(256, 128) for zz in zs], axis=1)
                right = jnp.concatenate([wgu[pl.ds(s, 128), :] for s in starts], axis=0)
                r = jnp.dot(left, right, preferred_element_type=F32)
                acc[some, pl.ds(self.h * TH, TH), :] += r.reshape(per, TH, 512)

        def late(self):
            for p in range(2):
                self.half2_in[p].wait()
                self.row_sib(p, 2, self.row_in[p, 2])

        def own_rows(self, n):
            for p in range(2):
                self.mul(p, c, n)

        def sib_rows(self, n):
            for p in range(2):
                for batch in ((0,), (1,), (2,), (0, 1), (0, 1, 2))[n]:
                    self.row_in[p, batch].wait()
                self.mul(p, oc, n)

        def sib_z(self, n):
            for batch in ((0,), (1,), (0, 1))[n]:
                self.zsib_in[batch].wait()
            self.mulz(oc, n)

        def hidden(self):
            h = self.h
            rows = pl.ds(h * TH, TH)

            @pl.loop(0, 16)
            def _(q):
                for e in range(2):
                    gate = acc[q, rows, e * 256 : e * 256 + 128]
                    upper = acc[q, rows, e * 256 + 128 : e * 256 + 256]
                    value = gate / (1.0 + jnp.exp(-gate)) * upper * wcol[q, rows, e * 128 : (e + 1) * 128]
                    value = value.astype(BF16)
                    hid[h, c, 0, q, :, e * 128 : (e + 1) * 128] = value[:RH]
                    hid[h, c, 1, q, :, e * 128 : (e + 1) * 128] = value[RH:]

            self.hid_in = recvs(hid.at[h, c])
            put(hid.at[h, c], hid.at[h, c], sibling, sends(hid.at[h, c]), self.hid_in)

    ka, kb = y * oc + x * c, x * oc + y * c

    def along(other, d):
        u, v = d * c, d * oc
        if other:
            return (lax.rem(y + 4 + u, 4), lax.rem(x + 4 + v, 4), z, c)
        return (lax.rem(y + 4 + v, 4), lax.rem(x + 4 + u, 4), z, c)

    def down(left, right, start, size):
        return jnp.dot(left, wd[0, :, lanes(start, size)], preferred_element_type=F32) + jnp.dot(
            right, wd[1, :, lanes(start, size)], preferred_element_type=F32
        )

    def add(*refs):
        total = refs[0][...].astype(F32)
        for ref in refs[1:]:
            total += ref[...].astype(F32)
        refs[0][...] = total.astype(BF16)

    order = (2, 1, -1, 0)
    side = (lax.broadcasted_iota(jnp.int32, (16 * RH, 128), 1) < 64) == (c == 0)

    class Sum:
        def __init__(self, h):
            self.h = h
            self.routes = (
                (ca.at[h], r1a.at[h], r2a.at[h], t1a.at[h], t2a.at[h], za.at[h], ka, kb, WIDTHS[0],
                 lambda d: along(False, d), lambda d: along(True, d)),
                (cb.at[h], r1b.at[h], r2b.at[h], t1b.at[h], t2b.at[h], zb.at[h], kb, ka, WIDTHS[1],
                 lambda d: along(True, d), lambda d: along(False, d)),
            )
            self.hid = hid.at[h]
            self.cc, self.q = cc.at[h], [None, q1.at[h], q2.at[h], q3.at[h], q4.at[h]]
            self.st1 = [(sends(r[1]), recvs(r[1])) for r in self.routes]
            self.ind = [(sends(r[2].at[0]), recvs(r[2].at[0])) for r in self.routes]
            self.dep_out = [sends(r[2].at[0]) for r in self.routes]
            self.dep_in = {(p, b): recvs(self.routes[p][2].at[0, 0]) for p in range(2) for b in order}
            self.st2 = [(sends(r[3]), recvs(r[3])) for r in self.routes]
            self.t2 = [(sends(r[4]), recvs(r[4])) for r in self.routes]
            self.zr = [(sends(r[5]), recvs(r[5])) for r in self.routes]
            self.q_out = [None] + [sends(q) for q in self.q[1:]]
            self.q_in = [None] + [(recvs(q.at[0]), recvs(q.at[1])) for q in self.q[1:]]
            self.xy = (sends(xcr.at[h]), recvs(xcr.at[h]))

        def cut(self, p):
            half = self.routes[p][8] * 4
            return pl.ds(0, half), pl.ds(half, half)

        def product(self, p):
            buf, size = self.routes[p][0], self.routes[p][8]
            left = self.hid[0, p].reshape(16 * RH, 256)
            right = self.hid[1, p].reshape(16 * RH, 256)
            for zz in range(8):
                r = down(left, right, zz * 896 + c * 512, size).astype(BF16)
                for q in range(16):
                    a, b = q // 4, q % 4
                    k, i = (a * oc + b * c, b * oc + a * c) if p == 0 else (b * oc + a * c, a * oc + b * c)
                    buf[k, i, :, zz * size : (zz + 1) * size] = r[q * RH : (q + 1) * RH]

        def begin(self, p):
            buf, r1, r2, t1, t2, zr, k, i, size, m2, m1 = self.routes[p]
            left, right = self.cut(p)
            self.product(p)
            put(buf.at[m4(k, 2), :, :, left], r1.at[0], m2(1), *self.st1[p])
            put(buf.at[m4(k, 2), :, :, right], r1.at[1], m2(-1), *self.st1[p])

        def independent(self, p):
            buf, r1, r2, t1, t2, zr, k, i, size, m2, m1 = self.routes[p]
            left, right = self.cut(p)
            put(buf.at[m4(k, 1), :, :, right], r2.at[0, :, :, right], m2(1), *self.ind[p])
            put(buf.at[m4(k, -1), :, :, left], r2.at[1, :, :, left], m2(-1), *self.ind[p])

        def columns(self, zs):
            lo = [self.hid[n, 0].reshape(16 * RH, 256) for n in range(2)]
            hi = [self.hid[n, 1].reshape(16 * RH, 256) for n in range(2)]

            def weights(*starts):
                return [jnp.concatenate([wd[n, :, lanes(s, 128)] for s in starts], axis=1) for n in range(2)]

            def dot(left, right):
                return jnp.dot(left[0], right[0], preferred_element_type=F32) + jnp.dot(left[1], right[1], preferred_element_type=F32)

            r_lo = dot(lo, weights(*(zz * 896 + 384 for zz in zs)))
            for n, zz in enumerate(zs):
                r = dot(hi, weights(zz * 896 + c * 512 + 256, zz * 896 + 384))
                self.cc[zz, :, :, 0:128] = r[:, :128].reshape(16, RH, 128).astype(BF16)
                r = jnp.where(side, r_lo[:, n * 128 : (n + 1) * 128], pltpu.roll(r[:, 128:], 64, 1))
                self.cc[zz, :, :, 128:256] = r.reshape(16, RH, 128).astype(BF16)

        def first_columns(self):
            first, second = pl.ds(0, 8), pl.ds(8, 8)
            cc_, q = self.cc, self.q
            self.columns((m8(z, 4), m8(z, 3)))
            put(cc_.at[m8(z, 4), first], q[1].at[0], dev(dz=1), self.q_out[1], self.q_in[1][0])
            put(cc_.at[m8(z, 4), second], q[1].at[1], dev(dz=-1), self.q_out[1], self.q_in[1][1])
            put(cc_.at[m8(z, 3), second], q[2].at[0, second], dev(dz=1), self.q_out[2], self.q_in[2][0])
            self.columns((m8(z, -3), m8(z, 2)))
            put(cc_.at[m8(z, -3), first], q[2].at[1, first], dev(dz=-1), self.q_out[2], self.q_in[2][1])

        def last_columns(self):
            self.columns((m8(z, -2), m8(z, 1)))
            self.columns((m8(z, -1), z))

        def z_second(self):
            first, second = pl.ds(0, 8), pl.ds(8, 8)
            cc_, q = self.cc, self.q
            self.q_in[1][0].wait()
            add(cc_.at[m8(z, 3), first], q[1].at[0])
            put(cc_.at[m8(z, 3), first], q[2].at[0, first], dev(dz=1), self.q_out[2], self.q_in[2][0])
            self.q_in[1][1].wait()
            add(cc_.at[m8(z, -3), second], q[1].at[1])
            put(cc_.at[m8(z, -3), second], q[2].at[1, second], dev(dz=-1), self.q_out[2], self.q_in[2][1])

        def z_next(self, t):
            for n, d in enumerate((1, -1)):
                self.q_in[t][n].wait()
                ref = self.cc.at[m8(z, d * (4 - t))]
                add(ref, self.q[t].at[n])
                put(ref, self.q[t + 1].at[n], dev(dz=d), self.q_out[t + 1], self.q_in[t + 1][n])

        def z_end(self):
            self.q_in[4][0].wait()
            self.q_in[4][1].wait()
            add(self.cc.at[z], self.q[4].at[0], self.q[4].at[1])
            for n, (dy, dx) in enumerate(plane):
                to = m4(y, dy) * 4 + m4(x, dx)
                put(self.cc.at[z, to], xcr.at[self.h, n], dev(dy, dx), *self.xy)

        def depend(self, p):
            buf, r1, r2, t1, t2, zr, k, i, size, m2, m1 = self.routes[p]
            left, right = self.cut(p)
            self.st1[p][1].wait()
            for b in order:
                j = m4(i, b)
                ref = buf.at[m4(k, 1), j, :, left]
                add(ref, r1.at[0, j])
                put(ref, r2.at[0, j, :, left], m2(1), self.dep_out[p], self.dep_in[p, b])
                ref = buf.at[m4(k, -1), j, :, right]
                add(ref, r1.at[1, j])
                put(ref, r2.at[1, j, :, right], m2(-1), self.dep_out[p], self.dep_in[p, b])

        def second(self, *blocks):
            for b in blocks:
                for p, (buf, r1, r2, t1, t2, zr, k, i, size, m2, m1) in enumerate(self.routes):
                    left, right = self.cut(p)
                    if b == 2:
                        self.ind[p][1].wait()
                    self.dep_in[p, b].wait()
                    j = m4(i, b)
                    add(buf.at[k, j], r2.at[0, j], r2.at[1, j])
                    if b == 2:
                        put(buf.at[k, j, :, left], t1.at[0], m1(1), *self.st2[p])
                        put(buf.at[k, j, :, right], t1.at[1], m1(-1), *self.st2[p])
                    elif b == 1:
                        put(buf.at[k, j, :, right], t2.at[0, :, right], m1(1), *self.t2[p])
                    elif b == -1:
                        put(buf.at[k, j, :, left], t2.at[1, :, left], m1(-1), *self.t2[p])

        def third(self):
            for p, (buf, r1, r2, t1, t2, zr, k, i, size, m2, m1) in enumerate(self.routes):
                left, right = self.cut(p)
                self.st2[p][1].wait()
                ref = buf.at[k, m4(i, 1), :, left]
                add(ref, t1.at[0])
                put(ref, t2.at[0, :, left], m1(1), *self.t2[p])
                ref = buf.at[k, m4(i, -1), :, right]
                add(ref, t1.at[1])
                put(ref, t2.at[1, :, right], m1(-1), *self.t2[p])

        def fourth(self):
            for p, (buf, r1, r2, t1, t2, zr, k, i, size, m2, m1) in enumerate(self.routes):
                self.t2[p][1].wait()
                add(buf.at[k, i], t2.at[0], t2.at[1])
                for d in (4, 3, -3, 2, -2, 1, -1):
                    n = d - 1 if d > 0 else d + 7
                    put(buf.at[k, i, :, lanes(m8(z, d) * size, size)], zr.at[n], dev(dz=d), *self.zr[p])

        def finish(self):
            h = self.h
            self.xy[1].wait()
            fc = self.cc[z, g].astype(F32)
            for n in range(15):
                fc += xcr[h, n].astype(F32)
            total = []
            for p, (buf, r1, r2, t1, t2, zr, k, i, size, m2, m1) in enumerate(self.routes):
                self.zr[p][1].wait()
                f = buf[k, i, :, lanes(z * size, size)].astype(F32)
                for d in range(7):
                    f += zr[d].astype(F32)
                total.append(f)
            fa, fb = total
            mixed = fc[:, 128:]
            turned = pltpu.roll(mixed, 64, 1)
            upper = jnp.concatenate([fb, fc[:, :128]], axis=1)
            one, two = slice(h * TH, h * TH + RH), slice(h * TH + RH, (h + 1) * TH)

            @pl.when(c == 0)
            def _():
                out[one, :] = jnp.concatenate([fa, mixed], axis=1)[:, :448].astype(BF16)
                out[two, :] = jnp.concatenate([upper, turned], axis=1)[:, :448].astype(BF16)

            @pl.when(c == 1)
            def _():
                out[one, :] = pltpu.roll(jnp.concatenate([mixed, fa], axis=1), 448, 1)[:, :448].astype(BF16)
                out[two, :] = pltpu.roll(jnp.concatenate([turned, upper], axis=1), 448, 1)[:, :448].astype(BF16)

    G = [Gather(h) for h in everyone]
    S = [Sum(h) for h in everyone]
    loads_in = [pltpu.make_async_copy(wgu, wgu, wsem), pltpu.make_async_copy(wd.at[c], wd.at[c], dsem)]

    def run(*steps):
        for n, step in enumerate(steps):
            call, rest = (step[0], step[1:]) if isinstance(step, tuple) else (step, ())
            mark(n, call, rest)
            call(*rest)

    def exchanged(h):
        G[h].hid_in.wait()

    a, b = G
    s, t = S
    run(
        a.begin_pieces, a.begin_first, a.begin_second, routing,
        a.pieces, a.firsts, b.begin_pieces, loads_in[0].wait, loads_in[1].wait,
        a.halves, (a.pass_on, 0), b.begin_first, (a.z_step, 1), (a.own_rows, 0),
        (a.pass_on, -1), routing_done, (a.pass_on, 1), b.begin_second, (a.sib_rows, 0), (a.z_step, 2), (a.pass_on, 2),
        b.pieces, (a.own_rows, 1), (a.mulz, c, 0), (a.sib_z, 0), b.firsts, (a.z_step, 3), (a.sib_rows, 1),
        a.late, (a.own_rows, 2), (b.z_step, 1), (a.z_step, 4), b.halves, (b.pass_on, 0), (a.mulz, c, 1),
        (b.own_rows, 0), (b.pass_on, -1), (a.sib_rows, 2), (b.pass_on, 1), (a.sib_z, 1), a.hidden,
        (b.z_step, 2), (b.pass_on, 2), (b.own_rows, 1), down_in.wait, (exchanged, 0),
        s.first_columns, (s.begin, 0), (s.begin, 1), (s.independent, 0), (s.independent, 1), (b.z_step, 3), b.late,
        (b.own_rows, 2), s.z_second, s.last_columns, (b.sib_rows, 4), (b.z_step, 4),
        (b.mulz, c, 2), (s.depend, 0), (s.depend, 1), (s.z_next, 2), (b.sib_z, 2), b.hidden,
        (exchanged, 1), t.first_columns, (s.second, 2), (t.begin, 0), (s.second, 1, -1, 0), (t.begin, 1),
        t.last_columns, t.z_second, (s.z_next, 3), s.third, (t.independent, 0), (t.independent, 1), (t.depend, 0), (t.depend, 1),
        (t.z_next, 2), s.z_end, s.fourth, (t.second, 2), (t.z_next, 3), (t.second, 1, -1, 0), t.third, t.z_end,
        t.fourth, s.finish, t.finish,
    )
    mark("b30_sends")
    for batch in send_waits:
        batch.wait()
    mark(None)


def local(tokens, gate_scores, expert_ids, gate_weight, up_weight, down_weight):
    vmem = pl.BlockSpec(memory_space=pltpu.VMEM)
    anywhere = pl.BlockSpec(memory_space=pl.ANY)

    def bf16(*shape):
        return pltpu.VMEM((CHUNKS, *shape), BF16)

    def route(size):
        w = 8 * size
        return [bf16(2, 4, RH, w // 2), bf16(2, 4, RH, w), bf16(2, RH, w // 2), bf16(2, RH, w), bf16(7, RH, size)]

    return pl.pallas_call(
        kernel,
        out_shape=jax.ShapeDtypeStruct((64, 448), BF16),
        in_specs=[anywhere, vmem, vmem, anywhere, anywhere, anywhere],
        out_specs=vmem,
        scratch_shapes=[
            bf16(2, 16, TH, PART),
            bf16(2, 16, TH, PART),
            bf16(2, 8, 16, TH, 128),
            pltpu.VMEM((7168, 512), BF16),
            pltpu.VMEM((2, 256, 7168), BF16),
            pltpu.VMEM((16, 64, 512), F32),
            pltpu.VMEM((16, 8, 128), F32),
            pltpu.VMEM((16, 8, 128), F32),
            pltpu.VMEM((16, 64, 256), F32),
            bf16(2, 2, 16, RH, 256),
            bf16(4, 4, RH, 8 * WIDTHS[0]),
            bf16(4, 4, RH, 8 * WIDTHS[1]),
            bf16(8, 16, RH, 256),
            *route(WIDTHS[0]),
            *route(WIDTHS[1]),
            bf16(2, 8, RH, 256),
            bf16(2, 16, RH, 256),
            bf16(2, 16, RH, 256),
            bf16(2, 16, RH, 256),
            bf16(15, RH, 256),
            pltpu.SemaphoreType.DMA((SENDS,)),
            pltpu.SemaphoreType.DMA((RECVS,)),
            pltpu.SemaphoreType.DMA((3 * CHUNKS + 2,)),
        ],
        compiler_params=pltpu.CompilerParams(
            collective_id=0, has_side_effects=True, vmem_limit_bytes=67043328
        ),
    )(tokens, gate_scores.T, expert_ids.T, gate_weight, up_weight, down_weight)


def solution(mesh):
    torus = Mesh(mesh.devices.reshape(4, 4, 8, 2), ("y", "x", "z", "c"))
    return jax.shard_map(
        local,
        mesh=torus,
        in_specs=(
            P(("y", "x"), None),
            P(("y", "x"), None),
            P(("y", "x"), None),
            P(("y", "x"), None, ("z", "c")),
            P(("y", "x"), None, ("z", "c")),
            P(("y", "x"), ("z", "c"), None),
        ),
        out_specs=P(("y", "x"), ("z", "c")),
        check_vma=False,
    )
```
